32 devices in a mesh: fsdp: 16 (over z, y, core), dp: 2 (over x).
Axes of the slice: x: 2, y: 2, z: 4, core: 2. Of those that a mesh axis runs over, the one named last changes fastest.
Arguments:
- block_input: bfloat16 [160, 416, 768], P(('fsdp', 'dp')), may hold values from -6 to 6
- segment_ids: int32 [160, 416], P(('fsdp', 'dp')), may hold values from -1 to 24, as said below
- ln1_gain: bfloat16 [768], P('fsdp'), may hold values from 0.099609375 to 1.8984375
- ln1_bias: bfloat16 [768], P('fsdp'), may hold values from -3 to 3
- qkv_weight: bfloat16 [768, 2304], P('fsdp'), may hold values from -0.21875 to 0.21875
- qv_bias: bfloat16 [1536], P('fsdp'), may hold values from -3 to 3
- out_weight: bfloat16 [768, 768], P('fsdp'), may hold values from -0.875 to 0.875
- out_bias: bfloat16 [768], P('fsdp'), may hold values from -3 to 3
- ln2_gain: bfloat16 [768], P('fsdp'), may hold values from 0.099609375 to 1.8984375
- ln2_bias: bfloat16 [768], P('fsdp'), may hold values from -3 to 3
- up_weight: bfloat16 [768, 3072], P('fsdp'), may hold values from -0.21875 to 0.21875
- up_bias: bfloat16 [3072], P('fsdp'), may hold values from -3 to 3
- down_weight: bfloat16 [3072, 768], P('fsdp'), may hold values from -0.109375 to 0.109375
- down_bias: bfloat16 [768], P('fsdp'), may hold values from -3 to 3
- out_cotangent: bfloat16 [160, 416, 768], P(('fsdp', 'dp')), may hold values from -6 to 6
Outputs:
- block_output: bfloat16 [160, 416, 768], P(('fsdp', 'dp'))
- input_grad: bfloat16 [160, 416, 768], P(('fsdp', 'dp'))
- ln1_gain_grad: float32 [768], P('fsdp')
- ln1_bias_grad: float32 [768], P('fsdp')
- qkv_weight_grad: float32 [768, 2304], P('fsdp')
- qv_bias_grad: float32 [1536], P('fsdp')
- out_weight_grad: float32 [768, 768], P('fsdp')
- out_bias_grad: float32 [768], P('fsdp')
- ln2_gain_grad: float32 [768], P('fsdp')
- ln2_bias_grad: float32 [768], P('fsdp')
- up_weight_grad: float32 [768, 3072], P('fsdp')
- up_bias_grad: float32 [3072], P('fsdp')
- down_weight_grad: float32 [3072, 768], P('fsdp')
- down_bias_grad: float32 [768], P('fsdp')
The draws below stay inside these ranges and needn't reach their ends.
Inputs may be any that keep to these rules, and one draw needn't show every extreme that they name: `segment_ids`: each packed row holds whole images of h x w slots with h and w from 4 to 14, numbered 0, 1, 2 in order from the row's start, followed by padding slots marked -1 (at least one in every row); some row holds the most images that fit.
All inputs are finite; a program needn't handle non-finite values.
Results may differ from the reference program's by a relative error of at most 0.013.
Values may be sent and summed in bfloat16 or wider, within the bound.
A program may use at most 256 MiB of HBM per device.

```python
import jax
import jax.numpy as jnp
from jax import lax

D = 768
HEADS = 12
HEAD_DIM = 64
FF = 3072
SLOTS = 416
SIDE_LO = 4
SIDE_HI = 14
ROWS = 160


def draw_segment_ids(key, part):
    first, second = jax.random.split(jax.random.fold_in(key, 17))
    count = SLOTS // (SIDE_LO * SIDE_LO) + 1
    heights = jax.random.randint(first, (ROWS, count), SIDE_LO, SIDE_HI + 1)
    widths = jax.random.randint(second, (ROWS, count), SIDE_LO, SIDE_HI + 1)
    row_index = jnp.arange(ROWS, dtype=jnp.int32)[:, None]
    heights = jnp.where(row_index == 0, SIDE_LO, heights)
    widths = jnp.where(row_index == 0, SIDE_LO, widths)
    ends = jnp.cumsum(heights * widths, axis=1)
    kept = ends <= SLOTS - 1
    filled = jnp.max(jnp.where(kept, ends, 0), axis=1)
    positions = jnp.arange(SLOTS, dtype=jnp.int32)
    number = jnp.sum((ends[:, None, :] <= positions[None, :, None]).astype(jnp.int32), axis=2)
    return jnp.where(positions[None, :] < filled[:, None], number, -1).astype(jnp.int32)


def steps_of(key, shape, cuts, least, largest):
    level, own = 1.0, jax.random.fold_in(key, 6)
    for position, shards_of in cuts:
        draws = jnp.exp(jax.random.uniform(jax.random.fold_in(own, position), (shards_of,), jnp.float32, least / len(cuts), largest / len(cuts)))
        level = level * jnp.repeat(draws, shape[position] // shards_of).reshape([-1 if axis == position else 1 for axis in range(len(shape))])
    return level


def gaussian(rng, shape, deviation, most, cuts=(), kind=jnp.bfloat16):
    array = deviation * jax.random.normal(rng, shape, jnp.float32)
    if cuts:
        array = array * steps_of(rng, shape, cuts, -0.22, 0.18)
    return jnp.clip(array, -most, most).astype(kind)


def setup_inputs(seed: int = 0) -> dict:
    splits = jax.random.split(jax.random.key(seed), 16)
    return {
        "block_input": gaussian(splits[0], (ROWS, SLOTS, D), 1.0, 6.0, ((0, 32),)),
        "segment_ids": draw_segment_ids(jax.random.fold_in(splits[15], 71), 0),
        "ln1_gain": jnp.clip(1.0 + 0.18 * jax.random.normal(splits[2], (D,), jnp.float32), 0.099609375, 1.8984375).astype(jnp.bfloat16),
        "ln1_bias": gaussian(splits[3], (D,), 0.5, 3.0, ((0, 16),)),
        "qkv_weight": gaussian(splits[4], (D, 3 * D), D ** -0.5, 0.21875, ((0, 16),)),
        "qv_bias": gaussian(splits[5], (2 * D,), 0.5, 3.0, ((0, 16),)),
        "out_weight": gaussian(splits[6], (D, D), (D // 16) ** -0.5, 0.875, ((0, 16),)),
        "out_bias": gaussian(splits[7], (D,), 0.5, 3.0, ((0, 16),)),
        "ln2_gain": jnp.clip(1.0 + 0.18 * jax.random.normal(splits[8], (D,), jnp.float32), 0.099609375, 1.8984375).astype(jnp.bfloat16),
        "ln2_bias": gaussian(splits[9], (D,), 0.5, 3.0, ((0, 16),)),
        "up_weight": gaussian(splits[10], (D, FF), D ** -0.5, 0.21875, ((0, 16),)),
        "up_bias": gaussian(splits[11], (FF,), 0.5, 3.0, ((0, 16),)),
        "down_weight": gaussian(splits[12], (FF, D), FF ** -0.5, 0.109375, ((0, 16),)),
        "down_bias": gaussian(splits[13], (D,), 0.5, 3.0, ((0, 16),)),
        "out_cotangent": gaussian(splits[14], (ROWS, SLOTS, D), 1.0, 6.0, ((0, 32),)),
    }


@jax.custom_vjp
def low(v):
    return lax.optimization_barrier(v.astype(jnp.bfloat16)).astype(jnp.float32)

@jax.custom_vjp
def low_back(v):
    return v

def low_keep(v):
    return (low(v), None)

def low_pass(kept, grad):
    return (grad,)

def back_keep(v):
    return (v, None)

def back_low(kept, grad):
    return (low(grad),)
low.defvjp(low_keep, low_pass)
low_back.defvjp(back_keep, back_low)

def matmul(left, right):
    return jnp.dot(left, right, preferred_element_type=jnp.float32, precision=lax.Precision.HIGHEST)

def layer_norm(values, gain, shift):
    center = values - lax.optimization_barrier(jnp.mean(values, axis=-1, keepdims=True))
    spread = lax.optimization_barrier(jnp.mean(center * center, axis=-1, keepdims=True))
    return center * lax.rsqrt(spread + 1e-06) * gain + shift

def row_attend(items):
    queries, keys_row, values_row, segment_row = items
    scores = jnp.einsum('qhe,khe->hqk', queries, keys_row, precision=lax.Precision.HIGHEST) * 0.125
    scores = low_back(scores)
    allowed = segment_row[:, None] == segment_row[None, :]
    scores = jnp.where(allowed[None], scores, -jnp.inf)
    highest = lax.optimization_barrier(jnp.max(scores, axis=-1, keepdims=True))
    expo = jnp.exp(scores - highest)
    probs = low(expo / lax.optimization_barrier(jnp.sum(expo, axis=-1, keepdims=True)))
    mixed = jnp.einsum('hqk,khe->qhe', probs, values_row, precision=lax.Precision.HIGHEST)
    return mixed.reshape(SLOTS, D)

def forward(params, inputs, segments):
    gain_one, shift_one, qkv_w, qv_b, proj_w, proj_b, gain_two, shift_two, up_w, up_b, down_w, down_b = params
    group = inputs.shape[0]
    flat = inputs.reshape(-1, D)
    normed = low(layer_norm(flat, gain_one, shift_one))
    projected = matmul(normed, qkv_w)
    queries = low(low_back(projected[:, :D] + qv_b[:D]))
    keys_all = low(low_back(projected[:, D:2 * D]))
    values_all = low(low_back(projected[:, 2 * D:] + qv_b[D:]))
    shape_four = (group, SLOTS, HEADS, HEAD_DIM)
    mixed = lax.map(jax.checkpoint(row_attend), (queries.reshape(shape_four), keys_all.reshape(shape_four), values_all.reshape(shape_four), segments))
    mixed = low(low_back(mixed.reshape(-1, D)))
    middle = flat + low_back(matmul(mixed, proj_w) + proj_b)
    normed_two = low(layer_norm(middle, gain_two, shift_two))
    pre = low_back(matmul(normed_two, up_w) + up_b)
    act = low(jax.nn.gelu(pre, approximate=False))
    branch = low_back(matmul(act, down_w) + down_b)
    return (middle + branch).reshape(inputs.shape)

def reference(block_input, segment_ids, ln1_gain, ln1_bias, qkv_weight, qv_bias, out_weight, out_bias, ln2_gain, ln2_bias, up_weight, up_bias, down_weight, down_bias, out_cotangent):
    params = tuple((item.astype(jnp.float32) for item in (ln1_gain, ln1_bias, qkv_weight, qv_bias, out_weight, out_bias, ln2_gain, ln2_bias, up_weight, up_bias, down_weight, down_bias)))
    group = 8
    count = ROWS // group
    inputs = block_input.astype(jnp.float32).reshape(count, group, SLOTS, D)
    segments = segment_ids.reshape(count, group, SLOTS)
    cotangents = out_cotangent.astype(jnp.float32).reshape(count, group, SLOTS, D)

    def step(total, items):
        xs, segs, cots = items
        result, pullback = jax.vjp(lambda prm, inp: forward(prm, inp, segs), params, xs)
        param_grads, input_grads = pullback(cots)
        total = jax.tree.map(jnp.add, total, param_grads)
        return (total, (result.astype(jnp.bfloat16), input_grads.astype(jnp.bfloat16)))
    zeros = tuple((jnp.zeros_like(item) for item in params))
    total, stacked = lax.scan(step, zeros, (inputs, segments, cotangents))
    outputs = stacked[0].reshape(ROWS, SLOTS, D)
    grads = stacked[1].reshape(ROWS, SLOTS, D)
    return (outputs, grads, total[0], total[1], total[2], total[3], total[4], total[5], total[6], total[7], total[8], total[9], total[10], total[11])
```

```python
import jax
import jax.numpy as jnp
from jax import lax
from jax.experimental import pallas as pl
from jax.experimental.pallas import tpu as pltpu
from jax.sharding import PartitionSpec as P

HEAD_DIM = 64
F32 = jnp.float32
BF16 = jnp.bfloat16
VMEM_LIMIT = 60 * 1024 * 1024
NT = (((1,), (1,)), ((), ()))
TN = (((0,), (0,)), ((), ()))


def dot(left, right):
    return jnp.dot(left, right, preferred_element_type=F32)


def dot_nt(left, right):
    return lax.dot_general(left, right, NT, preferred_element_type=F32)


def dot_tn(left, right):
    return lax.dot_general(left, right, TN, preferred_element_type=F32)


def norm_parts(values):
    center = values - jnp.mean(values, axis=-1, keepdims=True)
    inv = lax.rsqrt(jnp.mean(center * center, axis=-1, keepdims=True) + 1e-06)
    return center * inv, inv


def norm_grad(xhat, inv, grad, gain):
    scaled = grad * gain
    first = jnp.mean(scaled, axis=-1, keepdims=True)
    second = jnp.mean(scaled * xhat, axis=-1, keepdims=True)
    return inv * (scaled - first - xhat * second)


def half_masks(width):
    lane = lax.broadcasted_iota(jnp.int32, (1, width), 1)
    return (lane % (2 * HEAD_DIM)) < HEAD_DIM


def attn_fwd_kernel(
    x_ref, segc_ref, segr_ref, w_ref, gain_ref, shift_ref, bias_ref,
    h1_ref, qkv_ref, p_ref, mixed_ref, kz_ref, vt_ref, mt_ref, mask_ref,
):
    width = x_ref.shape[1]
    heads = width // HEAD_DIM
    xhat, _ = norm_parts(x_ref[...].astype(F32))
    h1 = (xhat * gain_ref[...] + shift_ref[...]).astype(BF16)
    h1_ref[...] = h1
    low = half_masks(width)
    q = (dot(h1, w_ref[:, :width]) + bias_ref[:, :width]).astype(BF16)
    qkv_ref[:, :width] = q * jnp.asarray(0.125, BF16)
    k = dot(h1, w_ref[:, width : 2 * width]).astype(BF16)
    qkv_ref[:, width : 2 * width] = k
    zero = jnp.zeros_like(k)
    kz_ref[0] = jnp.where(low, k, zero)
    kz_ref[1] = jnp.where(low, zero, k)
    v = (dot(h1, w_ref[:, 2 * width : 3 * width]) + bias_ref[:, width:]).astype(BF16)
    qkv_ref[:, 2 * width :] = v
    vt_ref[...] = v.T
    mask_ref[...] = jnp.where(segc_ref[...] == segr_ref[...], 0.0, -1e30)
    for head in range(heads):
        pair = slice(head // 2 * 128, head // 2 * 128 + 128)
        rows = slice(head * HEAD_DIM, (head + 1) * HEAD_DIM)
        scores = dot_nt(kz_ref[head % 2, :, pair], qkv_ref[:, pair]) + mask_ref[...]
        expo = jnp.exp(scores - jnp.max(scores, axis=0, keepdims=True))
        total = jnp.sum(expo, axis=0, keepdims=True)
        probs = (expo * (1.0 / total)).astype(BF16)
        p_ref[head] = probs
        mt_ref[rows, :] = dot(vt_ref[rows, :], probs)
    mixed_ref[...] = mt_ref[...].T.astype(BF16)


def attn_bwd_kernel(
    qkv_ref, p_ref, mixed_ref, do_ref, dproj_ref, dbias_ref, vz_ref, kt_ref, dqt_ref, d_ref,
):
    width = mixed_ref.shape[1]
    heads = width // HEAD_DIM
    low = half_masks(width)
    v = qkv_ref[:, 2 * width :]
    zero = jnp.zeros_like(v)
    vz_ref[0] = jnp.where(low, v, zero)
    vz_ref[1] = jnp.where(low, zero, v)
    kt_ref[...] = qkv_ref[:, width : 2 * width].T
    prod = (do_ref[...].astype(F32) * mixed_ref[...].astype(F32)).T
    d_ref[...] = jnp.sum(prod.reshape(heads, HEAD_DIM, prod.shape[1]), axis=1)
    low_pair = half_masks(2 * HEAD_DIM)
    for pair_index in range(heads // 2):
        pair = slice(pair_index * 128, pair_index * 128 + 128)
        dvs, dks = [], []
        for half in range(2):
            head = 2 * pair_index + half
            rows = slice(head * HEAD_DIM, (head + 1) * HEAD_DIM)
            dprobs = dot_nt(vz_ref[half, :, pair], do_ref[:, pair])
            probs = p_ref[head]
            dvs.append(dot(probs, do_ref[:, pair]))
            dscores = (probs.astype(F32) * (dprobs - d_ref[head : head + 1, :])).astype(BF16)
            dks.append(dot(dscores, qkv_ref[:, pair]))
            dqt_ref[rows, :] = dot(kt_ref[rows, :], dscores)
        start = width + pair_index * 128
        dproj_ref[:, start : start + 128] = jnp.where(low_pair, dks[0], dks[1]).astype(BF16)
        start = 2 * width + pair_index * 128
        dproj_ref[:, start : start + 128] = jnp.where(low_pair, dvs[0], dvs[1]).astype(BF16)
    dq = (dqt_ref[...] * 0.125).T.astype(BF16)
    dproj_ref[:, :width] = dq

    @pl.when(pl.program_id(0) == 0)
    def _():
        dbias_ref[...] = jnp.zeros_like(dbias_ref)

    dbias_ref[:, :width] += jnp.sum(dq.astype(F32), axis=0, keepdims=True)
    dbias_ref[:, width:] += jnp.sum(dproj_ref[:, 2 * width :].astype(F32), axis=0, keepdims=True)


def mlp_kernel(
    x_ref, att_ref, dy_ref, wo_ref, wu_ref, wd_ref, bo_ref, gain_ref, shift_ref, bu_ref, bd_ref,
    out_ref, h2_ref, act_ref, dpre_ref, dz_ref, datt_ref, dsmall_ref, dbu_ref,
):
    width = x_ref.shape[1]
    hidden = wu_ref.shape[1]
    chunk = 512 if hidden % 512 == 0 else 128
    middle = x_ref[...].astype(F32) + dot(att_ref[...], wo_ref[...]) + bo_ref[...]
    xhat, inv = norm_parts(middle)
    h2 = (xhat * gain_ref[...] + shift_ref[...]).astype(BF16)
    h2_ref[...] = h2
    dy = dy_ref[...]
    out = middle + bd_ref[...]
    dh2 = None

    @pl.when(pl.program_id(0) == 0)
    def _():
        dsmall_ref[...] = jnp.zeros_like(dsmall_ref)
        dbu_ref[...] = jnp.zeros_like(dbu_ref)

    for start in range(0, hidden, chunk):
        cols = slice(start, start + chunk)
        pre = dot(h2, wu_ref[:, cols]) + bu_ref[:, cols]
        dact = dot_nt(dy, wd_ref[cols, :])
        cdf = 0.5 * (1.0 + lax.erf(pre * 0.7071067811865476))
        pdf = jnp.exp(-0.5 * pre * pre) * 0.3989422804014327
        act = (pre * cdf).astype(BF16)
        dpre = dact * (cdf + pre * pdf)
        act_ref[:, cols] = act
        dbu_ref[:, cols] += jnp.sum(dpre, axis=0, keepdims=True)
        dpre = dpre.astype(BF16)
        dpre_ref[:, cols] = dpre
        out += dot(act, wd_ref[cols, :])
        part = dot_nt(dpre, wu_ref[:, cols])
        dh2 = part if dh2 is None else dh2 + part
    out_ref[...] = out.astype(BF16)
    wide_dy = dy.astype(F32)
    dmiddle = wide_dy + norm_grad(xhat, inv, dh2, gain_ref[...])
    dz = dmiddle.astype(BF16)
    dz_ref[...] = dz
    datt_ref[...] = dot_nt(dz, wo_ref[...]).astype(BF16)
    dsmall_ref[0:1, :] += jnp.sum(dz.astype(F32), axis=0, keepdims=True)
    dsmall_ref[1:2, :] += jnp.sum(dh2 * xhat, axis=0, keepdims=True)
    dsmall_ref[2:3, :] += jnp.sum(dh2, axis=0, keepdims=True)
    dsmall_ref[3:4, :] += jnp.sum(wide_dy, axis=0, keepdims=True)


def input_grad_kernel(x_ref, dproj_ref, dz_ref, w_ref, gain_ref, dx_ref, dsmall_ref):
    width = x_ref.shape[1]
    dh1 = dot_nt(dproj_ref[...], w_ref[:, : 3 * width])
    xhat, inv = norm_parts(x_ref[...].astype(F32))
    dx = dz_ref[...].astype(F32) + norm_grad(xhat, inv, dh1, gain_ref[...])
    dx_ref[...] = dx.astype(BF16)

    @pl.when(pl.program_id(0) == 0)
    def _():
        dsmall_ref[...] = jnp.zeros_like(dsmall_ref)

    dsmall_ref[0:1, :] += jnp.sum(dh1 * xhat, axis=0, keepdims=True)
    dsmall_ref[1:2, :] += jnp.sum(dh1, axis=0, keepdims=True)


def row_spec(*shape):
    return pl.BlockSpec((None,) + shape, lambda i: (i,) + (0,) * len(shape))


def whole(*shape):
    return pl.BlockSpec(shape, lambda i: (0,) * len(shape), pipeline_mode=pl.Buffered(1))


def acc_spec(*shape):
    return pl.BlockSpec(shape, lambda i: (0,) * len(shape))


def sds(shape, dtype):
    return jax.ShapeDtypeStruct(shape, dtype)


def run(kernel, grid, in_specs, outs, out_specs, scratch, args, flops, name):
    total = sum(a.size * a.dtype.itemsize for a in args)
    total += sum(o.size * jnp.dtype(o.dtype).itemsize for o in outs)
    return pl.pallas_call(
        kernel,
        grid=grid,
        in_specs=in_specs,
        out_specs=out_specs,
        out_shape=outs,
        scratch_shapes=scratch,
        compiler_params=pltpu.CompilerParams(
            dimension_semantics=("arbitrary",), vmem_limit_bytes=VMEM_LIMIT
        ),
        cost_estimate=pl.CostEstimate(flops=flops, bytes_accessed=total, transcendentals=0),
        name=name,
    )(*args)


def attn_fwd(x, segs, w, gain, shift, bias):
    rows, slots, width = x.shape
    heads = width // HEAD_DIM
    outs = (
        sds((rows, slots, width), BF16),
        sds((rows, slots, 3 * width), BF16),
        sds((rows, heads, slots, slots), BF16),
        sds((rows, slots, width), BF16),
    )
    return run(
        attn_fwd_kernel,
        (rows,),
        [
            row_spec(slots, width),
            row_spec(slots, 1),
            row_spec(1, slots),
            whole(width, 3 * width),
            whole(1, width),
            whole(1, width),
            whole(1, 2 * width),
        ],
        outs,
        [
            row_spec(slots, width),
            row_spec(slots, 3 * width),
            row_spec(heads, slots, slots),
            row_spec(slots, width),
        ],
        [
            pltpu.VMEM((2, slots, width), BF16),
            pltpu.VMEM((width, slots), BF16),
            pltpu.VMEM((width, slots), F32),
            pltpu.VMEM((slots, slots), F32),
        ],
        (x, segs[:, :, None], segs[:, None, :], w, gain, shift, bias),
        rows * (6 * slots * width * width + 4 * slots * slots * width * 4),
        "attn_fwd",
    )


def attn_bwd(qkv, probs, mixed, dmixed):
    rows, slots, width = mixed.shape
    heads = width // HEAD_DIM
    return run(
        attn_bwd_kernel,
        (rows,),
        [
            row_spec(slots, 3 * width),
            row_spec(heads, slots, slots),
            row_spec(slots, width),
            row_spec(slots, width),
        ],
        (sds((rows, slots, 3 * width), BF16), sds((1, 2 * width), F32)),
        [row_spec(slots, 3 * width), acc_spec(1, 2 * width)],
        [
            pltpu.VMEM((2, slots, width), BF16),
            pltpu.VMEM((width, slots), BF16),
            pltpu.VMEM((width, slots), F32),
            pltpu.VMEM((heads, slots), F32),
        ],
        (qkv, probs, mixed, dmixed),
        rows * 8 * slots * slots * width * 4,
        "attn_bwd",
    )


def mlp(x, mixed, dy, wo, wu, wd, bo, gain, shift, bu, bd):
    rows, slots, width = x.shape
    hidden = wu.shape[1]
    act = row_spec(slots, width)
    wide = row_spec(slots, hidden)
    return run(
        mlp_kernel,
        (rows,),
        [
            act, act, act,
            whole(width, width), whole(width, hidden), whole(hidden, width),
            whole(1, width), whole(1, width), whole(1, width), whole(1, hidden), whole(1, width),
        ],
        (
            sds(x.shape, BF16), sds(x.shape, BF16), sds((rows, slots, hidden), BF16),
            sds((rows, slots, hidden), BF16), sds(x.shape, BF16), sds(x.shape, BF16),
            sds((8, width), F32), sds((1, hidden), F32),
        ),
        [act, act, wide, wide, act, act, acc_spec(8, width), acc_spec(1, hidden)],
        [],
        (x, mixed, dy, wo, wu, wd, bo, gain, shift, bu, bd),
        rows * slots * width * (8 * hidden + 4 * width),
        "mlp",
    )


def input_grad(x, dproj, dz, w, gain):
    rows, slots, width = x.shape
    act = row_spec(slots, width)
    return run(
        input_grad_kernel,
        (rows,),
        [act, row_spec(slots, 3 * width), act, whole(width, 3 * width), whole(1, width)],
        (sds(x.shape, BF16), sds((8, width), F32)),
        [act, acc_spec(8, width)],
        [],
        (x, dproj, dz, w, gain),
        rows * slots * width * width * 6,
        "input_grad",
    )


def gather(shard):
    return lax.all_gather(shard, "fsdp", axis=0, tiled=True)


def scatter(full):
    owned = lax.psum_scatter(full, "fsdp", scatter_dimension=0, tiled=True)
    return lax.psum(owned, "dp").astype(F32)


def weight_grad(left, right):
    flat_left = left.reshape(-1, left.shape[-1])
    flat_right = right.reshape(-1, right.shape[-1])
    return dot_tn(flat_left, flat_right).astype(BF16)


def per_device(
    block_input, segment_ids, ln1_gain, ln1_bias, qkv_weight, qv_bias, out_weight, out_bias,
    ln2_gain, ln2_bias, up_weight, up_bias, down_weight, down_bias, out_cotangent,
):
    rows, slots, width = block_input.shape
    shard = ln1_gain.shape[0]
    parts = width // shard
    small = jnp.concatenate(
        [
            ln1_gain, ln1_bias, qv_bias, out_bias, ln2_gain, ln2_bias, up_bias, down_bias,
        ]
    )[None]
    sizes = [shard, shard, 2 * shard, shard, shard, shard, 4 * shard, shard]
    small_full = gather(small).astype(F32)
    vectors, start = [], 0
    for size in sizes:
        vectors.append(small_full[:, start : start + size].reshape(1, size * parts))
        start += size
    gain1, shift1, bias_qv, bias_out, gain2, shift2, bias_up, bias_down = vectors
    w_qkv = gather(qkv_weight)
    w_out = gather(out_weight)
    w_up = gather(up_weight)
    w_down = gather(down_weight)

    h1, qkv, probs, mixed = attn_fwd(block_input, segment_ids, w_qkv, gain1, shift1, bias_qv)
    out, h2, act, dpre, dz, dmixed, dsmall2, dbias_up = mlp(
        block_input, mixed, out_cotangent, w_out, w_up, w_down,
        bias_out, gain2, shift2, bias_up, bias_down,
    )
    down_grad = scatter(weight_grad(act, out_cotangent))
    up_grad = scatter(weight_grad(h2, dpre))
    out_grad = scatter(weight_grad(mixed, dz))
    dproj, dbias_qv = attn_bwd(qkv, probs, mixed, dmixed)
    qkv_grad = scatter(weight_grad(h1, dproj))
    dx, dsmall1 = input_grad(block_input, dproj, dz, w_qkv, gain1)
    grads = [
        dsmall1[0:1], dsmall1[1:2], dbias_qv, dsmall2[0:1],
        dsmall2[1:2], dsmall2[2:3], dbias_up, dsmall2[3:4],
    ]
    packed = jnp.concatenate([g.reshape(parts, -1) for g in grads], axis=1)
    owned = lax.psum_scatter(packed, "fsdp", scatter_dimension=0, tiled=True)
    owned = lax.psum(owned, "dp")[0]
    pieces, start = [], 0
    for size in sizes:
        pieces.append(owned[start : start + size])
        start += size
    return (
        out, dx, pieces[0], pieces[1], qkv_grad, pieces[2], out_grad, pieces[3],
        pieces[4], pieces[5], up_grad, pieces[6], down_grad, pieces[7],
    )


def solution(mesh):
    both = ("fsdp", "dp")
    vec, mat, act = P("fsdp"), P("fsdp", None), P(both, None, None)
    return jax.shard_map(
        per_device,
        mesh=mesh,
        in_specs=(
            act, P(both, None), vec, vec, mat, vec, mat, vec, vec, vec, mat, vec, mat, vec, act,
        ),
        out_specs=(act, act, vec, vec, mat, vec, mat, vec, vec, vec, mat, vec, mat, vec),
        check_vma=False,
    )
```

```python
import functools

import jax
import jax.numpy as jnp
from jax import lax
from jax.experimental import pallas as pl
from jax.experimental.pallas import tpu as pltpu
from jax.sharding import PartitionSpec as P

HEAD_DIM = 64
F32 = jnp.float32
BF16 = jnp.bfloat16
VMEM_LIMIT = 60 * 1024 * 1024
NT = (((1,), (1,)), ((), ()))
TN = (((0,), (0,)), ((), ()))


def dot(left, right):
    return jnp.dot(left, right, preferred_element_type=F32)


def dot_nt(left, right):
    return lax.dot_general(left, right, NT, preferred_element_type=F32)


def dot_tn(left, right):
    return lax.dot_general(left, right, TN, preferred_element_type=F32)


def norm_parts(values):
    center = values - jnp.mean(values, axis=-1, keepdims=True)
    inv = lax.rsqrt(jnp.mean(center * center, axis=-1, keepdims=True) + 1e-06)
    return center * inv, inv


def norm_grad(xhat, inv, grad, gain):
    scaled = grad * gain
    first = jnp.mean(scaled, axis=-1, keepdims=True)
    second = jnp.mean(scaled * xhat, axis=-1, keepdims=True)
    return inv * (scaled - first - xhat * second)


def half_masks(width):
    lane = lax.broadcasted_iota(jnp.int32, (1, width), 1)
    return (lane % (2 * HEAD_DIM)) < HEAD_DIM


def attn_fwd_row(
    x_ref, segc_ref, segr_ref, w_ref, small_ref,
    h1_ref, qkv_ref, p_ref, mixed_ref, kz_ref, vt_ref, mt_ref, mask_ref, hook,
):
    width = x_ref.shape[1]
    heads = width // HEAD_DIM
    xhat, _ = norm_parts(x_ref[...].astype(F32))
    h1 = (xhat * small_ref[0:1, :] + small_ref[1:2, :]).astype(BF16)
    h1_ref[...] = h1
    low = half_masks(width)
    q = (dot(h1, w_ref[:, :width]) + small_ref[8:9, :]).astype(BF16)
    qkv_ref[:, :width] = q * jnp.asarray(0.125, BF16)
    k = dot(h1, w_ref[:, width : 2 * width]).astype(BF16)
    qkv_ref[:, width : 2 * width] = k
    zero = jnp.zeros_like(k)
    kz_ref[0] = jnp.where(low, k, zero)
    kz_ref[1] = jnp.where(low, zero, k)
    v = (dot(h1, w_ref[:, 2 * width :]) + small_ref[9:10, :]).astype(BF16)
    qkv_ref[:, 2 * width :] = v
    vt_ref[...] = v.T
    mask_ref[...] = jnp.where(segc_ref[...] == segr_ref[...], 0.0, -1e30)
    hook(0)
    for head in range(heads):
        pair = slice(head // 2 * 128, head // 2 * 128 + 128)
        rows = slice(head * HEAD_DIM, (head + 1) * HEAD_DIM)
        scores = dot_nt(kz_ref[head % 2, :, pair], qkv_ref[:, pair]) + mask_ref[...]
        expo = jnp.exp(scores - jnp.max(scores, axis=0, keepdims=True))
        total = jnp.sum(expo, axis=0, keepdims=True)
        probs = (expo * (1.0 / total)).astype(BF16)
        p_ref[head] = probs
        mt_ref[rows, :] = dot(vt_ref[rows, :], probs)
        if head in (3, 7):
            hook(1 + head // 4)
    mixed_ref[...] = mt_ref[...].T.astype(BF16)
    hook(3)


def attn_fwd_kernel(
    x_ref, segc_ref, segr_ref, w_ref, small_ref,
    h1_ref, qkv_ref, p_ref, mixed_ref, kz_ref, vt_ref, mt_ref, mask_ref,
):
    attn_fwd_row(
        x_ref, segc_ref, segr_ref, w_ref, small_ref,
        h1_ref, qkv_ref, p_ref, mixed_ref, kz_ref, vt_ref, mt_ref, mask_ref, lambda point: None,
    )


class Place:
    def __init__(self):
        fsdp = lax.axis_index("fsdp")
        self.fsdp = fsdp
        self.z = fsdp // 4
        self.y = (fsdp // 2) % 2
        self.c = fsdp % 2
        self.x = lax.axis_index("dp")

    def device(self, z=None, y=None, c=None, x=None):
        z = self.z if z is None else z
        y = self.y if y is None else y
        c = self.c if c is None else c
        x = self.x if x is None else x
        return {"fsdp": (z * 2 + y) * 2 + c, "dp": x}

    def greet(self):
        barrier = pltpu.get_barrier_semaphore()

        def signal(device):
            pl.semaphore_signal(
                barrier, inc=1, device_id=device, device_id_type=pl.DeviceIdType.MESH
            )

        signal(self.device(c=1 - self.c))
        signal(self.device(y=1 - self.y))
        signal(self.device(x=1 - self.x))

        @pl.when(self.z > 0)
        def _():
            signal(self.device(z=self.z - 1))

        @pl.when(self.z < 3)
        def _():
            signal(self.device(z=self.z + 1))

        upper = jnp.where(self.z > 0, 1, 0)
        lower = jnp.where(self.z < 3, 1, 0)
        pl.semaphore_wait(barrier, 3 + upper + lower)


RELS = [(0, 0)] + [(d, h) for d in range(2) for h in range(1, 4)]
GATHER_SLOTS = 41


class Gather:
    def __init__(self, place, index, dst, own, send, recv, local):
        self.place, self.index, self.dst, self.own = place, index, dst, own
        self.send, self.recv, self.local = send, recv, local
        self.rows, self.cols = own.shape

    def source_z(self, rel):
        d, h = rel
        return self.place.z - h if d == 0 else self.place.z + h

    def exists(self, rel):
        d, h = rel
        if h == 0:
            return None
        return self.place.z >= h if d == 0 else self.place.z + h <= 3

    def guard(self, rel, body):
        cond = self.exists(rel)
        if cond is None:
            body()
        else:
            pl.when(cond)(body)

    def view(self, ref, start, half):
        if half is None:
            return ref.at[pl.ds(start, self.rows), :]
        width = self.cols // 2
        first = pl.multiple_of(half * width, 128)
        return ref.at[pl.ds(start, self.rows), pl.ds(first, width)]

    def copy(self, slot, rel, y, c, half, device, own=False):
        index = (self.source_z(rel) * 2 + y) * 2 + c
        start = pl.multiple_of(index * self.rows, self.rows)
        view = self.view(self.dst, start, half)
        src = self.view(self.own, 0, half) if own else view
        return pltpu.make_async_remote_copy(
            src_ref=src,
            dst_ref=view,
            send_sem=self.send.at[self.index, slot],
            recv_sem=self.recv.at[self.index, slot],
            device_id=device,
            device_id_type=pl.DeviceIdType.MESH,
        )

    def z_copy(self, d, rel, own=False):
        place = self.place
        target = place.z + 1 if d == 0 else place.z - 1
        return self.copy(
            d * 3 + rel[1], rel, place.y, place.c, None, place.device(z=target), own
        )

    def z_room(self, d):
        return self.place.z < 3 if d == 0 else self.place.z > 0

    def y_copy(self, rel, own=False):
        place = self.place
        return self.copy(
            6 + RELS.index(rel), rel, place.y, place.c, place.x, place.device(y=1 - place.y), own
        )

    def x_copy(self, rel):
        place = self.place
        return self.copy(
            13 + RELS.index(rel), rel, 1 - place.y, place.c, place.x, place.device(x=1 - place.x)
        )

    def c_copy(self, rel, own=False):
        place = self.place
        return self.copy(
            20 + RELS.index(rel), rel, place.y, place.c, None, place.device(c=1 - place.c), own
        )

    def cy_copy(self, rel, k):
        place = self.place
        half = place.x if k == 0 else 1 - place.x
        return self.copy(
            27 + 2 * RELS.index(rel) + k, rel, 1 - place.y, place.c, half,
            place.device(c=1 - place.c),
        )

    def local_copy(self):
        start = pl.multiple_of(self.place.fsdp * self.rows, self.rows)
        return pltpu.make_async_copy(
            self.own, self.dst.at[pl.ds(start, self.rows), :], self.local.at[self.index]
        )

    def begin(self):
        own = (0, 0)
        for d in range(2):
            pl.when(self.z_room(d))(lambda d=d: self.z_copy(d, own, True).start())
        self.y_copy(own, True).start()
        self.c_copy(own, True).start()
        self.local_copy().start()

    def arrived(self, slot, rel, y, c, half):
        self.copy(slot, rel, y, c, half, self.place.device()).wait_recv()

    def on_z(self, rel):
        d, h = rel

        def body():
            place = self.place
            self.arrived(d * 3 + h - 1, rel, place.y, place.c, None)
            if h < 3:
                pl.when(self.z_room(d))(lambda: self.z_copy(d, rel).start())
            self.y_copy(rel).start()
            self.c_copy(rel).start()

        self.guard(rel, body)

    def on_y(self, rel):
        def body():
            place = self.place
            self.arrived(6 + RELS.index(rel), rel, 1 - place.y, place.c, place.x)
            self.x_copy(rel).start()
            self.cy_copy(rel, 0).start()

        self.guard(rel, body)

    def on_x(self, rel):
        def body():
            place = self.place
            self.arrived(13 + RELS.index(rel), rel, 1 - place.y, place.c, 1 - place.x)
            self.cy_copy(rel, 1).start()

        self.guard(rel, body)

    def events(self):
        up, down = [(0, h) for h in range(1, 4)], [(1, h) for h in range(1, 4)]
        own = (0, 0)
        return [
            lambda: (self.on_z(up[0]), self.on_z(down[0])),
            lambda: self.on_y(own),
            lambda: (self.on_z(up[1]), self.on_z(down[1])),
            lambda: (self.on_y(up[0]), self.on_y(down[0])),
            lambda: self.on_x(own),
            lambda: (self.on_z(up[2]), self.on_z(down[2])),
            lambda: (self.on_y(up[1]), self.on_y(down[1])),
            lambda: (self.on_x(up[0]), self.on_x(down[0])),
            lambda: (self.on_y(up[2]), self.on_y(down[2])),
            lambda: (self.on_x(up[1]), self.on_x(down[1])),
            lambda: (self.on_x(up[2]), self.on_x(down[2])),
        ]

    def finish_recv(self):
        place = self.place
        self.local_copy().wait()
        for rel in RELS:

            def body(rel=rel):
                number = RELS.index(rel)
                self.arrived(20 + number, rel, place.y, 1 - place.c, None)
                self.arrived(27 + 2 * number, rel, 1 - place.y, 1 - place.c, place.x)
                self.arrived(28 + 2 * number, rel, 1 - place.y, 1 - place.c, 1 - place.x)

            self.guard(rel, body)

    def finish_send(self):
        for rel in RELS:

            def body(rel=rel):
                d, h = rel
                for way in range(2) if h == 0 else (d,):
                    if h < 3:
                        pl.when(self.z_room(way))(
                            lambda way=way: self.z_copy(way, rel).wait_send()
                        )
                self.y_copy(rel).wait_send()
                self.x_copy(rel).wait_send()
                self.c_copy(rel).wait_send()
                self.cy_copy(rel, 0).wait_send()
                self.cy_copy(rel, 1).wait_send()

            self.guard(rel, body)


def place_small(one_ref, two_ref, four_ref, shard, fsdp):
    width = one_ref.shape[1]
    per_row = width // shard
    rows = lax.broadcasted_iota(jnp.int32, (8, width), 0)
    ones = pltpu.roll(one_ref[...], fsdp * shard, 1)
    two = pltpu.roll(two_ref[...], (fsdp * 2 % per_row) * shard, 1)
    four = pltpu.roll(four_ref[...], (fsdp * 4 % per_row) * shard, 1)
    two = jnp.where(rows == fsdp * 2 // per_row, two, 0.0)
    four = jnp.where(rows == 2 + fsdp * 4 // per_row, four, 0.0)
    return jnp.concatenate([ones, two + four], axis=0)


def gather_attn_kernel(
    x_ref, segc_ref, segr_ref, one_ref, two_ref, four_ref,
    qkv_own, out_own, up_own, down_own,
    h1_ref, qkv_ref, p_ref, mixed_ref, small_ref, wq_hbm, out_hbm, up_hbm, down_hbm,
    wq_ref, tiny_own, tiny_ref, kz_ref, vt_ref, mt_ref, mask_ref, send, recv, local,
):
    place = Place()
    row = pl.program_id(0)
    last = pl.num_programs(0) - 1
    parts = wq_ref.shape[0] // qkv_own.shape[0]
    tiny = Gather(place, 0, tiny_ref, tiny_own, send, recv, local)
    first = Gather(place, 1, wq_ref, qkv_own, send, recv, local)
    rest = [
        Gather(place, 2 + i, dst, own, send, recv, local)
        for i, (dst, own) in enumerate(
            ((up_hbm, up_own), (down_hbm, down_own), (out_hbm, out_own))
        )
    ]
    keep = pltpu.make_async_copy(wq_ref, wq_hbm, local.at[5])

    @pl.when(row == 0)
    def _():
        tiny_own[...] = place_small(one_ref, two_ref, four_ref, qkv_own.shape[0], place.fsdp).astype(BF16)
        place.greet()
        tiny.begin()
        first.begin()
        early, main = tiny.events(), first.events()
        for step in range(len(main)):
            early[step]()
            main[step]()
            if step == 5:
                for item in rest:
                    item.begin()
        tiny.finish_recv()
        total = tiny_ref[0:16, :].astype(F32)
        for index in range(1, parts):
            total += tiny_ref[16 * index : 16 * index + 16, :].astype(F32)
        small_ref[...] = total
        first.finish_recv()
        keep.start()

    queue = [event for item in rest for event in item.events()]
    points = 4 * 5 - 1
    share = -(-len(queue) // points)

    def hook(point):
        for r in range(5):
            number = r * 4 + point
            todo = queue[number * share : (number + 1) * share]
            if todo:

                @pl.when(row == r)
                def _(todo=todo):
                    for event in todo:
                        event()

    attn_fwd_row(
        x_ref, segc_ref, segr_ref, wq_ref, small_ref,
        h1_ref, qkv_ref, p_ref, mixed_ref, kz_ref, vt_ref, mt_ref, mask_ref, hook,
    )

    @pl.when(row == last)
    def _():
        keep.wait()
        for item in rest:
            item.finish_recv()
        for item in [tiny, first] + rest:
            item.finish_send()


def attn_bwd_kernel(
    qkv_ref, p_ref, mixed_ref, do_ref, dproj_ref, dbias_ref, vz_ref, kt_ref, dqt_ref, d_ref,
):
    width = mixed_ref.shape[1]
    heads = width // HEAD_DIM
    low = half_masks(width)
    v = qkv_ref[:, 2 * width :]
    zero = jnp.zeros_like(v)
    vz_ref[0] = jnp.where(low, v, zero)
    vz_ref[1] = jnp.where(low, zero, v)
    kt_ref[...] = qkv_ref[:, width : 2 * width].T
    prod = (do_ref[...].astype(F32) * mixed_ref[...].astype(F32)).T
    d_ref[...] = jnp.sum(prod.reshape(heads, HEAD_DIM, prod.shape[1]), axis=1)
    low_pair = half_masks(2 * HEAD_DIM)
    for pair_index in range(heads // 2):
        pair = slice(pair_index * 128, pair_index * 128 + 128)
        dvs, dks = [], []
        for half in range(2):
            head = 2 * pair_index + half
            rows = slice(head * HEAD_DIM, (head + 1) * HEAD_DIM)
            dprobs = dot_nt(vz_ref[half, :, pair], do_ref[:, pair])
            probs = p_ref[head]
            dvs.append(dot(probs, do_ref[:, pair]))
            dscores = (probs.astype(F32) * (dprobs - d_ref[head : head + 1, :])).astype(BF16)
            dks.append(dot(dscores, qkv_ref[:, pair]))
            dqt_ref[rows, :] = dot(kt_ref[rows, :], dscores)
        start = width + pair_index * 128
        dproj_ref[:, start : start + 128] = jnp.where(low_pair, dks[0], dks[1]).astype(BF16)
        start = 2 * width + pair_index * 128
        dproj_ref[:, start : start + 128] = jnp.where(low_pair, dvs[0], dvs[1]).astype(BF16)
    dq = (dqt_ref[...] * 0.125).T.astype(BF16)
    dproj_ref[:, :width] = dq

    @pl.when(pl.program_id(0) == 0)
    def _():
        dbias_ref[...] = jnp.zeros_like(dbias_ref)

    dbias_ref[:, :width] += jnp.sum(dq.astype(F32), axis=0, keepdims=True)
    dbias_ref[:, width:] += jnp.sum(dproj_ref[:, 2 * width :].astype(F32), axis=0, keepdims=True)


def mlp_kernel(
    x_ref, att_ref, dy_ref, wo_ref, wu_ref, wd_ref, small_ref,
    out_ref, h2_ref, act_ref, dpre_ref, dz_ref, datt_ref, dsmall_ref, dbu_ref,
):
    width = x_ref.shape[1]
    hidden = wu_ref.shape[1]
    gain, shift = small_ref[3:4, :], small_ref[4:5, :]
    middle = x_ref[...].astype(F32) + dot(att_ref[...], wo_ref[...]) + small_ref[2:3, :]
    xhat, inv = norm_parts(middle)
    h2 = (xhat * gain + shift).astype(BF16)
    h2_ref[...] = h2
    dy = dy_ref[...]
    out = middle + small_ref[5:6, :]
    dh2 = None

    @pl.when(pl.program_id(0) == 0)
    def _():
        dsmall_ref[...] = jnp.zeros_like(dsmall_ref)
        dbu_ref[...] = jnp.zeros_like(dbu_ref)

    for part_index in range(hidden // width):
        cols = slice(part_index * width, (part_index + 1) * width)
        pre = dot(h2, wu_ref[:, cols]) + small_ref[10 + part_index : 11 + part_index, :]
        dact = dot_nt(dy, wd_ref[cols, :])
        cdf = 0.5 * (1.0 + lax.erf(pre * 0.7071067811865476))
        pdf = jnp.exp(-0.5 * pre * pre) * 0.3989422804014327
        act = (pre * cdf).astype(BF16)
        dpre = dact * (cdf + pre * pdf)
        act_ref[:, cols] = act
        dbu_ref[:, cols] += jnp.sum(dpre, axis=0, keepdims=True)
        dpre = dpre.astype(BF16)
        dpre_ref[:, cols] = dpre
        out += dot(act, wd_ref[cols, :])
        part = dot_nt(dpre, wu_ref[:, cols])
        dh2 = part if dh2 is None else dh2 + part
    out_ref[...] = out.astype(BF16)
    wide_dy = dy.astype(F32)
    dmiddle = wide_dy + norm_grad(xhat, inv, dh2, gain)
    dz = dmiddle.astype(BF16)
    dz_ref[...] = dz
    datt_ref[...] = dot_nt(dz, wo_ref[...]).astype(BF16)
    dsmall_ref[0:1, :] += jnp.sum(dz.astype(F32), axis=0, keepdims=True)
    dsmall_ref[1:2, :] += jnp.sum(dh2 * xhat, axis=0, keepdims=True)
    dsmall_ref[2:3, :] += jnp.sum(dh2, axis=0, keepdims=True)
    dsmall_ref[3:4, :] += jnp.sum(wide_dy, axis=0, keepdims=True)


def input_grad_kernel(x_ref, dproj_ref, dz_ref, w_ref, small_ref, dx_ref, dsmall_ref):
    width = x_ref.shape[1]
    dh1 = dot_nt(dproj_ref[...], w_ref[:, : 3 * width])
    xhat, inv = norm_parts(x_ref[...].astype(F32))
    dx = dz_ref[...].astype(F32) + norm_grad(xhat, inv, dh1, small_ref[0:1, :])
    dx_ref[...] = dx.astype(BF16)

    @pl.when(pl.program_id(0) == 0)
    def _():
        dsmall_ref[...] = jnp.zeros_like(dsmall_ref)

    dsmall_ref[0:1, :] += jnp.sum(dh1 * xhat, axis=0, keepdims=True)
    dsmall_ref[1:2, :] += jnp.sum(dh1, axis=0, keepdims=True)


def row_spec(*shape):
    return pl.BlockSpec((None,) + shape, lambda i: (i,) + (0,) * len(shape))


def whole(*shape):
    return pl.BlockSpec(shape, lambda i: (0,) * len(shape), pipeline_mode=pl.Buffered(1))


def acc_spec(*shape):
    return pl.BlockSpec(shape, lambda i: (0,) * len(shape))


def sds(shape, dtype):
    return jax.ShapeDtypeStruct(shape, dtype)


def run(kernel, grid, in_specs, outs, out_specs, scratch, args, flops, name, collective_id=None):
    total = sum(a.size * a.dtype.itemsize for a in args)
    total += sum(o.size * jnp.dtype(o.dtype).itemsize for o in outs)
    return pl.pallas_call(
        kernel,
        grid=grid,
        in_specs=in_specs,
        out_specs=out_specs,
        out_shape=outs,
        scratch_shapes=scratch,
        compiler_params=pltpu.CompilerParams(
            dimension_semantics=("arbitrary",),
            vmem_limit_bytes=VMEM_LIMIT,
            collective_id=collective_id,
            has_side_effects=collective_id is not None,
        ),
        cost_estimate=pl.CostEstimate(flops=flops, bytes_accessed=total, transcendentals=0),
        name=name,
    )(*args)


def attn_outs(rows, slots, width, heads):
    outs = (
        sds((rows, slots, width), BF16),
        sds((rows, slots, 3 * width), BF16),
        sds((rows, heads, slots, slots), BF16),
        sds((rows, slots, width), BF16),
    )
    specs = [
        row_spec(slots, width),
        row_spec(slots, 3 * width),
        row_spec(heads, slots, slots),
        row_spec(slots, width),
    ]
    scratch = [
        pltpu.VMEM((2, slots, width), BF16),
        pltpu.VMEM((width, slots), BF16),
        pltpu.VMEM((width, slots), F32),
        pltpu.VMEM((slots, slots), F32),
    ]
    return outs, specs, scratch


def attn_flops(rows, slots, width):
    return rows * (6 * slots * width * width + 4 * slots * slots * width * 4)


def attn_fwd(x, segs, w, small):
    rows, slots, width = x.shape
    outs, specs, scratch = attn_outs(rows, slots, width, width // HEAD_DIM)
    return run(
        attn_fwd_kernel,
        (rows,),
        [
            row_spec(slots, width), row_spec(slots, 1), row_spec(1, slots),
            whole(width, 3 * width), whole(16, width),
        ],
        outs,
        specs,
        scratch,
        (x, segs[:, :, None], segs[:, None, :], w, small),
        attn_flops(rows, slots, width),
        "attn_fwd",
    )


def gather_attn(x, segs, smalls, qkv_own, out_own, up_own, down_own):
    rows, slots, width = x.shape
    parts = width // qkv_own.shape[0]
    hidden = up_own.shape[1]
    outs, specs, scratch = attn_outs(rows, slots, width, width // HEAD_DIM)
    hbm = pl.BlockSpec(memory_space=pl.ANY)
    return run(
        gather_attn_kernel,
        (rows,),
        [row_spec(slots, width), row_spec(slots, 1), row_spec(1, slots)]
        + [whole(8, width)] * 3
        + [whole(*own.shape) for own in (qkv_own, out_own, up_own, down_own)],
        outs + (
            sds((16, width), F32), sds((width, 3 * width), BF16), sds((width, width), BF16),
            sds((width, hidden), BF16), sds((hidden, width), BF16),
        ),
        specs + [acc_spec(16, width), hbm, hbm, hbm, hbm],
        [
            pltpu.VMEM((width, 3 * width), BF16),
            pltpu.VMEM((16, width), BF16),
            pltpu.VMEM((16 * parts, width), BF16),
        ] + scratch + [
            pltpu.SemaphoreType.DMA((5, GATHER_SLOTS)),
            pltpu.SemaphoreType.DMA((5, GATHER_SLOTS)),
            pltpu.SemaphoreType.DMA((6,)),
        ],
        (x, segs[:, :, None], segs[:, None, :], *smalls, qkv_own, out_own, up_own, down_own),
        attn_flops(rows, slots, width),
        "gather_attn",
        collective_id=0,
    )


def attn_bwd(qkv, probs, mixed, dmixed):
    rows, slots, width = mixed.shape
    heads = width // HEAD_DIM
    return run(
        attn_bwd_kernel,
        (rows,),
        [
            row_spec(slots, 3 * width),
            row_spec(heads, slots, slots),
            row_spec(slots, width),
            row_spec(slots, width),
        ],
        (sds((rows, slots, 3 * width), BF16), sds((1, 2 * width), F32)),
        [row_spec(slots, 3 * width), acc_spec(1, 2 * width)],
        [
            pltpu.VMEM((2, slots, width), BF16),
            pltpu.VMEM((width, slots), BF16),
            pltpu.VMEM((width, slots), F32),
            pltpu.VMEM((heads, slots), F32),
        ],
        (qkv, probs, mixed, dmixed),
        rows * 8 * slots * slots * width * 4,
        "attn_bwd",
    )


def mlp(x, mixed, dy, wo, wu, wd, small):
    rows, slots, width = x.shape
    hidden = wu.shape[1]
    act = row_spec(slots, width)
    wide = row_spec(slots, hidden)
    return run(
        mlp_kernel,
        (rows,),
        [
            act, act, act,
            whole(width, width), whole(width, hidden), whole(hidden, width),
            whole(16, width),
        ],
        (
            sds(x.shape, BF16), sds(x.shape, BF16), sds((rows, slots, hidden), BF16),
            sds((rows, slots, hidden), BF16), sds(x.shape, BF16), sds(x.shape, BF16),
            sds((8, width), F32), sds((1, hidden), F32),
        ),
        [act, act, wide, wide, act, act, acc_spec(8, width), acc_spec(1, hidden)],
        [],
        (x, mixed, dy, wo, wu, wd, small),
        rows * slots * width * (8 * hidden + 4 * width),
        "mlp",
    )


def input_grad(x, dproj, dz, w, small):
    rows, slots, width = x.shape
    act = row_spec(slots, width)
    return run(
        input_grad_kernel,
        (rows,),
        [act, row_spec(slots, 3 * width), act, whole(width, 3 * width), whole(16, width)],
        (sds(x.shape, BF16), sds((8, width), F32)),
        [act, acc_spec(8, width)],
        [],
        (x, dproj, dz, w, small),
        rows * slots * width * width * 6,
        "input_grad",
    )


def gather(shard):
    return lax.all_gather(shard, "fsdp", axis=0, tiled=True)


def scatter(full):
    owned = lax.psum_scatter(full, "fsdp", scatter_dimension=0, tiled=True)
    return lax.psum(owned, "dp").astype(F32)


def weight_grad(left, right):
    flat_left = left.reshape(-1, left.shape[-1])
    flat_right = right.reshape(-1, right.shape[-1])
    return dot_tn(flat_left, flat_right).astype(BF16)


def per_device(
    linked, block_input, segment_ids, ln1_gain, ln1_bias, qkv_weight, qv_bias, out_weight, out_bias,
    ln2_gain, ln2_bias, up_weight, up_bias, down_weight, down_bias, out_cotangent,
):
    rows, slots, width = block_input.shape
    shard = ln1_gain.shape[0]
    parts = width // shard
    sizes = [shard, shard, 2 * shard, shard, shard, shard, 4 * shard, shard]
    ones = [ln1_gain, ln1_bias, out_bias, ln2_gain, ln2_bias, down_bias]
    if linked:

        def rows_of(vectors):
            padded = [jnp.pad(v.astype(F32), (0, width - v.shape[0])) for v in vectors]
            return jnp.stack(padded + [jnp.zeros((width,), F32)] * (8 - len(padded)))

        smalls = (rows_of(ones), rows_of([qv_bias] * 8), rows_of([up_bias] * 8))
        h1, qkv, probs, mixed, small, w_qkv, w_out, w_up, w_down = gather_attn(
            block_input, segment_ids, smalls, qkv_weight, out_weight, up_weight, down_weight
        )
    else:
        small = jnp.concatenate(
            [gather(v)[None] for v in ones]
            + [jnp.zeros((2, width), BF16)]
            + [gather(v).reshape(-1, width) for v in (qv_bias, up_bias)]
            + [jnp.zeros((2, width), BF16)]
        ).astype(F32)
        w_qkv = gather(qkv_weight)
        w_out = gather(out_weight)
        w_up = gather(up_weight)
        w_down = gather(down_weight)
        h1, qkv, probs, mixed = attn_fwd(block_input, segment_ids, w_qkv, small)
    out, h2, act, dpre, dz, dmixed, dsmall2, dbias_up = mlp(
        block_input, mixed, out_cotangent, w_out, w_up, w_down, small
    )
    down_grad = scatter(weight_grad(act, out_cotangent))
    up_grad = scatter(weight_grad(h2, dpre))
    out_grad = scatter(weight_grad(mixed, dz))
    dproj, dbias_qv = attn_bwd(qkv, probs, mixed, dmixed)
    qkv_grad = scatter(weight_grad(h1, dproj))
    dx, dsmall1 = input_grad(block_input, dproj, dz, w_qkv, small)
    grads = [
        dsmall1[0:1], dsmall1[1:2], dbias_qv, dsmall2[0:1],
        dsmall2[1:2], dsmall2[2:3], dbias_up, dsmall2[3:4],
    ]
    packed = jnp.concatenate([g.reshape(parts, -1) for g in grads], axis=1)
    owned = lax.psum_scatter(packed, "fsdp", scatter_dimension=0, tiled=True)
    owned = lax.psum(owned, "dp")[0]
    pieces, start = [], 0
    for size in sizes:
        pieces.append(owned[start : start + size])
        start += size
    return (
        out, dx, pieces[0], pieces[1], qkv_grad, pieces[2], out_grad, pieces[3],
        pieces[4], pieces[5], up_grad, pieces[6], down_grad, pieces[7],
    )


def solution(mesh):
    both = ("fsdp", "dp")
    linked = mesh.shape["fsdp"] == 16 and mesh.shape["dp"] == 2
    vec, mat, act = P("fsdp"), P("fsdp", None), P(both, None, None)
    return jax.shard_map(
        functools.partial(per_device, linked),
        mesh=mesh,
        in_specs=(
            act, P(both, None), vec, vec, mat, vec, mat, vec, vec, vec, mat, vec, mat, vec, act,
        ),
        out_specs=(act, act, vec, vec, mat, vec, mat, vec, vec, vec, mat, vec, mat, vec),
        check_vma=False,
    )
```
